16 devices in a mesh: dp: 2 (over z), cp: 8 (over y, x, core).
Axes of the slice: x: 2, y: 2, z: 2, core: 2. Of those that a mesh axis runs over, the one named last changes fastest.
Arguments:
- image: bfloat16 [16384, 3072], P(('dp', 'cp')), parts along dimension 0
- text: bfloat16 [1024, 3072], P('dp'), parts along dimension 0
- cond_vec: bfloat16 [2, 3072], P('dp'), parts along dimension 0
- rope_cos: float32 [16384, 64], P(('dp', 'cp')), parts along dimension 0
- rope_sin: float32 [16384, 64], P(('dp', 'cp')), parts along dimension 0
- w_mod: bfloat16 [2, 3072, 18432], replicated
- b_mod: float32 [2, 18432], replicated
- w_qkv: bfloat16 [2, 3072, 9216], replicated
- b_qkv: float32 [2, 9216], replicated
- qk_gain: float32 [2, 2, 128], replicated
- w_out: bfloat16 [2, 3072, 3072], replicated
- b_out: float32 [2, 3072], replicated
- w_up: bfloat16 [2, 3072, 12288], replicated
- b_up: float32 [2, 12288], replicated
- w_down: bfloat16 [2, 12288, 3072], replicated
- b_down: float32 [2, 3072], replicated
Outputs:
- output 1: bfloat16 [16384, 3072], P(('dp', 'cp')), parts along dimension 0
- output 2: bfloat16 [1024, 3072], P('dp'), parts along dimension 0
There are 2 independent parts. The reference program is written for one: setup_inputs(seed, part) draws one part's arguments, and reference() takes and returns one part's arrays. A program takes and returns all parts, laid end to end along the dimension named above; an argument that names none is the same for every part.
All inputs are finite; a program needn't handle non-finite values.
Results may differ from the reference program's by a relative error of at most 0.00756735.
Values are sent between devices in bfloat16 or wider.
A program may use at most 2.75 GiB of HBM per device.

```python
import jax
import jax.numpy as jnp
from jax import lax

HIDDEN = 3072
NUM_HEADS = 24
HEAD_DIM = 128
FF_DIM = 12288
TXT_LEN = 512
IMG_LEN = 8192
QUERY_BLOCK = 64
GRID_WIDTH = 64
REGIONS = 16
NORM_EPS = 1e-6
ROPE_THETA = 10000.0


def normal(key, shape, spread):
    return spread * jax.random.normal(key, shape, jnp.float32)


def rope_tables(key):
    keys = jax.random.split(key, 3)
    offset_t = jax.random.randint(keys[0], (), 0, 256)
    offset_h = jax.random.randint(keys[1], (), 0, 256)
    offset_w = jax.random.randint(keys[2], (), 0, 256)
    token = jnp.arange(IMG_LEN)
    dim_t = HEAD_DIM // 8
    dim_hw = (HEAD_DIM - dim_t) // 2
    omega_t = ROPE_THETA ** (-jnp.arange(0, dim_t, 2).astype(jnp.float32) / dim_t)
    omega_hw = ROPE_THETA ** (-jnp.arange(0, dim_hw, 2).astype(jnp.float32) / dim_hw)
    pos_t = jnp.zeros((IMG_LEN, 1), jnp.float32) + offset_t.astype(jnp.float32)
    pos_h = (token // GRID_WIDTH + offset_h).astype(jnp.float32)[:, None]
    pos_w = (token % GRID_WIDTH + offset_w).astype(jnp.float32)[:, None]
    angle = jnp.concatenate([pos_t * omega_t, pos_h * omega_hw, pos_w * omega_hw], axis=1)
    return jnp.cos(angle), jnp.sin(angle)


def setup_inputs(seed: int = 0, part: int = 0) -> dict:
    base = jax.random.key(seed)
    part_keys = jax.random.split(jax.random.fold_in(base, part), 5)
    shared = jax.random.split(jax.random.key(seed + 1), 11)
    region_vecs = normal(part_keys[0], (REGIONS, HIDDEN), 1.0)
    image = jnp.repeat(region_vecs, IMG_LEN // REGIONS, axis=0) + normal(part_keys[1], (IMG_LEN, HIDDEN), 0.4)
    text = normal(part_keys[2], (TXT_LEN, HIDDEN), 1.0)
    cond_vec = normal(part_keys[3], (1, HIDDEN), 1.0)
    rope_cos, rope_sin = rope_tables(part_keys[4])
    hid_scale = HIDDEN ** -0.5
    return dict(
        image=image.astype(jnp.bfloat16),
        text=text.astype(jnp.bfloat16),
        cond_vec=cond_vec.astype(jnp.bfloat16),
        rope_cos=rope_cos,
        rope_sin=rope_sin,
        w_mod=normal(shared[0], (2, HIDDEN, 6 * HIDDEN), hid_scale).astype(jnp.bfloat16),
        b_mod=normal(shared[1], (2, 6 * HIDDEN), 0.5),
        w_qkv=normal(shared[2], (2, HIDDEN, 3 * HIDDEN), hid_scale).astype(jnp.bfloat16),
        b_qkv=normal(shared[3], (2, 3 * HIDDEN), 0.3),
        qk_gain=1.4 + normal(shared[4], (2, 2, HEAD_DIM), 0.2),
        w_out=normal(shared[5], (2, HIDDEN, HIDDEN), hid_scale).astype(jnp.bfloat16),
        b_out=normal(shared[6], (2, HIDDEN), 0.3),
        w_up=normal(shared[7], (2, HIDDEN, FF_DIM), hid_scale).astype(jnp.bfloat16),
        b_up=normal(shared[8], (2, FF_DIM), 0.3),
        w_down=normal(shared[9], (2, FF_DIM, HIDDEN), FF_DIM ** -0.5).astype(jnp.bfloat16),
        b_down=normal(shared[10], (2, HIDDEN), 0.3),
    )


def layer_norm(rows):
    mean = jnp.mean(rows, axis=-1, keepdims=True)
    centered = rows - mean
    return centered * lax.rsqrt(jnp.mean(centered * centered, axis=-1, keepdims=True) + NORM_EPS)


def rms_norm(rows, gain):
    return rows * lax.rsqrt(jnp.mean(rows * rows, axis=-1, keepdims=True) + NORM_EPS) * gain


def apply_rope(rows, rope_cos, rope_sin):
    half = rows.shape[-1] // 2
    cos_b = rope_cos[:, None, :]
    sin_b = rope_sin[:, None, :]
    first = rows[..., :half]
    second = rows[..., half:]
    return jnp.concatenate([first * cos_b - second * sin_b, second * cos_b + first * sin_b], axis=-1)


def branch_qkv(rows, mod_row, w_qkv, b_qkv, gains):
    normed = (layer_norm(rows.astype(jnp.float32)) * (1.0 + mod_row[HIDDEN:2 * HIDDEN]) + mod_row[0:HIDDEN]).astype(jnp.bfloat16)
    qkv_rows = (jnp.dot(normed, w_qkv, preferred_element_type=jnp.float32) + b_qkv).astype(jnp.bfloat16)
    qkv_rows = qkv_rows.reshape(rows.shape[0], 3, NUM_HEADS, HEAD_DIM)
    queries = rms_norm(qkv_rows[:, 0].astype(jnp.float32), gains[0])
    keys = rms_norm(qkv_rows[:, 1].astype(jnp.float32), gains[1])
    return queries, keys, qkv_rows[:, 2]


def branch_out(rows, attended, mod_row, w_out, b_out, w_up, b_up, w_down, b_down):
    residual = rows.astype(jnp.float32) + mod_row[2 * HIDDEN:3 * HIDDEN] * (jnp.dot(attended, w_out, preferred_element_type=jnp.float32) + b_out)
    normed = (layer_norm(residual) * (1.0 + mod_row[4 * HIDDEN:5 * HIDDEN]) + mod_row[3 * HIDDEN:4 * HIDDEN]).astype(jnp.bfloat16)
    inner = jax.nn.gelu(jnp.dot(normed, w_up, preferred_element_type=jnp.float32) + b_up, approximate=True).astype(jnp.bfloat16)
    return (residual + mod_row[5 * HIDDEN:6 * HIDDEN] * (jnp.dot(inner, w_down, preferred_element_type=jnp.float32) + b_down)).astype(jnp.bfloat16)


def attend(queries, keys, values):
    scores = jnp.einsum('qhd,khd->hqk', queries, keys) * (HEAD_DIM ** -0.5)
    peak = jnp.max(scores, axis=-1, keepdims=True)
    weights = jnp.exp(scores - peak)
    total = jnp.sum(weights, axis=-1)
    summed = jnp.einsum('hqk,khd->qhd', weights, values)
    return summed / jnp.transpose(total)[:, :, None]


def reference(image, text, cond_vec, rope_cos, rope_sin, w_mod, b_mod, w_qkv, b_qkv, qk_gain, w_out, b_out, w_up, b_up, w_down, b_down):
    activated = jax.nn.silu(cond_vec.astype(jnp.float32)).astype(jnp.bfloat16)
    mod_img = jnp.dot(activated, w_mod[0], preferred_element_type=jnp.float32)[0] + b_mod[0]
    mod_txt = jnp.dot(activated, w_mod[1], preferred_element_type=jnp.float32)[0] + b_mod[1]
    q_img, k_img, v_img = branch_qkv(image, mod_img, w_qkv[0], b_qkv[0], qk_gain[0])
    q_img = apply_rope(q_img, rope_cos, rope_sin).astype(jnp.bfloat16)
    k_img = apply_rope(k_img, rope_cos, rope_sin).astype(jnp.bfloat16)
    q_txt, k_txt, v_txt = branch_qkv(text, mod_txt, w_qkv[1], b_qkv[1], qk_gain[1])
    q_txt = q_txt.astype(jnp.bfloat16)
    all_keys = jnp.concatenate([k_txt.astype(jnp.bfloat16), k_img], axis=0).astype(jnp.float32)
    all_values = jnp.concatenate([v_txt, v_img], axis=0).astype(jnp.float32)

    def image_block(block_q):
        return attend(block_q, all_keys, all_values)

    img_queries = q_img.astype(jnp.float32).reshape(IMG_LEN // QUERY_BLOCK, QUERY_BLOCK, NUM_HEADS, HEAD_DIM)
    img_att = lax.map(image_block, img_queries).reshape(IMG_LEN, HIDDEN).astype(jnp.bfloat16)

    def text_head(triple):
        return attend(triple[0], triple[1], triple[2])

    head_major = (jnp.swapaxes(q_txt.astype(jnp.float32), 0, 1)[:, :, None, :],
                  jnp.swapaxes(all_keys, 0, 1)[:, :, None, :],
                  jnp.swapaxes(all_values, 0, 1)[:, :, None, :])
    txt_att = jnp.swapaxes(lax.map(text_head, head_major)[:, :, 0, :], 0, 1).reshape(TXT_LEN, HIDDEN).astype(jnp.bfloat16)
    image_out = branch_out(image, img_att, mod_img, w_out[0], b_out[0], w_up[0], b_up[0], w_down[0], b_down[0])
    text_out = branch_out(text, txt_att, mod_txt, w_out[1], b_out[1], w_up[1], b_up[1], w_down[1], b_down[1])
    return image_out, text_out
```

```python
import functools

import jax
import jax.numpy as jnp
from jax import lax
from jax.experimental import pallas as pl
from jax.experimental.pallas import tpu as pltpu
from jax.sharding import PartitionSpec as P

NORM_EPS = 1e-6
HEAD = 128
LOG2E = 1.4426950408889634
SAFE_SCORE = 60.0
SAFE_VALUE = 1e6


def params(dims):
    return pltpu.CompilerParams(dimension_semantics=("arbitrary",) * dims, vmem_limit_bytes=60 * 2**20)


def cost(flops, moved, trans=0):
    return pl.CostEstimate(flops=flops, bytes_accessed=moved, transcendentals=trans)


def whole_block(shape):
    return pl.BlockSpec(shape, lambda *_: (0,) * len(shape))


def layer_norm(rows):
    mean = jnp.mean(rows, axis=-1, keepdims=True)
    centered = rows - mean
    return centered * lax.rsqrt(jnp.mean(centered * centered, axis=-1, keepdims=True) + NORM_EPS)


def mod_kernel(me_ref, act_ref, w_ref, out_ref):
    out_ref[0] = jnp.dot(act_ref[...], w_ref[0], preferred_element_type=jnp.float32)


def mod_columns(me, activated, w_mod, group):
    branches, hidden, width = w_mod.shape
    share = width // group
    step = share // 3
    rows = activated.shape[0]
    return pl.pallas_call(
        mod_kernel,
        out_shape=jax.ShapeDtypeStruct((branches, rows, share), jnp.float32),
        grid_spec=pltpu.PrefetchScalarGridSpec(
            num_scalar_prefetch=1, grid=(branches, 3),
            in_specs=[whole_block((rows, hidden)),
                      pl.BlockSpec((1, hidden, step), lambda b, n, me: (b, 0, me[0] * 3 + n))],
            out_specs=pl.BlockSpec((1, rows, step), lambda b, n, me: (b, 0, n))),
        compiler_params=params(2), cost_estimate=cost(2 * branches * rows * hidden * share, 2 * branches * hidden * share),
        name="modulate",
    )(me, activated, w_mod)


def head_norm(t, gain):
    x = t.astype(jnp.bfloat16).astype(jnp.float32)
    return x * lax.rsqrt(jnp.mean(x * x, axis=-1, keepdims=True) + NORM_EPS) * gain


def image_qkv_kernel(me_ref, h_ref, *refs, per, tile):
    w_refs, b_refs = refs[:per], refs[per:2 * per]
    gain_ref, cos_ref, sin_ref = refs[2 * per:2 * per + 3]
    outs = refs[2 * per + 3:]
    half, t = pl.program_id(0), pl.program_id(1)
    rows = h_ref.shape[0]

    def run(kind, group):
        weights = jnp.concatenate([w[0] for w in w_refs], axis=1)
        bias = jnp.concatenate([b[0] for b in b_refs], axis=1)
        for m in range(rows // tile):
            sl = pl.ds(m * tile, tile)
            acc = jnp.dot(h_ref[sl, :], weights, preferred_element_type=jnp.float32) + bias
            for i in range(per):
                piece = acc[:, i * HEAD:(i + 1) * HEAD]
                if kind == "v":
                    res = piece
                else:
                    y = head_norm(piece, gain_ref[0])
                    res = y * cos_ref[sl, :] + pltpu.roll(y, HEAD // 2, 1) * sin_ref[sl, :]
                outs[group * per + i][0, sl, :] = res.astype(jnp.bfloat16)

    for group in range(len(outs) // per):
        @pl.when(jnp.logical_and(half == group, t < 2))
        def _():
            run("qk", group)

        @pl.when(jnp.logical_and(half == group, t == 2))
        def _():
            run("v", group)


def image_qkv(me, h, w_qkv, b_qkv, gains, cos, sin, slot, group):
    rows, hidden = h.shape
    heads = hidden // HEAD
    per = 4
    halves = group // per

    def col(i):
        return lambda half, t, me: (0, 0, t * heads + slot * group + jnp.bitwise_xor(me[0], half * per + i))

    def out_map(own):
        def index(half, t, me):
            return (jnp.where(half < own, 0, jnp.where(half == own, t, 2)), 0, 0)
        return index

    return pl.pallas_call(
        functools.partial(image_qkv_kernel, per=per, tile=256),
        out_shape=[jax.ShapeDtypeStruct((3, rows, HEAD), jnp.bfloat16)] * group,
        grid_spec=pltpu.PrefetchScalarGridSpec(
            num_scalar_prefetch=1, grid=(halves, 3),
            in_specs=[whole_block((rows, hidden))]
            + [pl.BlockSpec((1, hidden, HEAD), col(i)) for i in range(per)]
            + [pl.BlockSpec((1, 1, HEAD), col(i)) for i in range(per)]
            + [pl.BlockSpec((1, 1, HEAD), lambda half, t, me: (jnp.minimum(t, 1), 0, 0)),
               whole_block((rows, HEAD)), whole_block((rows, HEAD))],
            out_specs=[pl.BlockSpec((1, rows, HEAD), out_map(s // per)) for s in range(group)]),
        compiler_params=params(2), cost_estimate=cost(2 * rows * hidden * 3 * group * HEAD, 2 * hidden * 3 * group * HEAD),
        name="image_qkv",
    )(me, h, *([w_qkv] * per), *([b_qkv] * per), gains, cos, sin)


def text_qkv_kernel(me_ref, h_ref, w_ref, b_ref, gain_ref, out_ref):
    t = pl.program_id(1)
    acc = jnp.dot(h_ref[...], w_ref[0], preferred_element_type=jnp.float32) + b_ref[0]
    normed = head_norm(acc, gain_ref[0])
    out_ref[0, 0] = jnp.where(t < 2, normed, acc).astype(jnp.bfloat16)


def text_qkv(me, h, w_qkv, b_qkv, gains, slots, group):
    rows, hidden = h.shape
    heads = hidden // HEAD

    def col(j, t, me):
        return (1, 0, t * heads + j * group + me[0])

    return pl.pallas_call(
        text_qkv_kernel,
        out_shape=jax.ShapeDtypeStruct((slots, 3, rows, HEAD), jnp.bfloat16),
        grid_spec=pltpu.PrefetchScalarGridSpec(
            num_scalar_prefetch=1, grid=(slots, 3),
            in_specs=[whole_block((rows, hidden)), pl.BlockSpec((1, hidden, HEAD), col), pl.BlockSpec((1, 1, HEAD), col),
                      pl.BlockSpec((1, 1, HEAD), lambda j, t, me: (jnp.minimum(t, 1), 0, 0))],
            out_specs=pl.BlockSpec((1, 1, rows, HEAD), lambda j, t, me: (j, t, 0, 0))),
        compiler_params=params(2), cost_estimate=cost(2 * rows * hidden * 3 * slots * HEAD, 2 * hidden * 3 * slots * HEAD),
        name="text_qkv",
    )(me, h, w_qkv, b_qkv, gains)


def attend_kernel(bound_ref, *refs, n_src, blk, kb):
    srcs, tref = refs[:n_src], refs[n_src]
    outs, tout = refs[n_src + 1:2 * n_src + 1], refs[2 * n_src + 1]
    qt, ks, vt, flag = refs[2 * n_src + 2:]
    b = pl.program_id(0)
    keys = ks.shape[0]
    rows = srcs[0].shape[1]
    scale2 = LOG2E * HEAD ** -0.5

    @pl.when(b == 0)
    def _():
        vmax = jnp.zeros((8, HEAD), jnp.float32)
        pos = 0
        for ref in (tref,) + tuple(srcs):
            for c in range(ref.shape[1] // blk):
                sl = pl.ds(c * blk, blk)
                qt[pos // blk] = ref[0, sl, :].T
                ks[pl.ds(pos, blk), :] = ref[1, sl, :]
                v = ref[2, sl, :]
                vt[:, pl.ds(pos, blk)] = v.T
                vmax = jnp.maximum(vmax, jnp.max(jnp.abs(v.astype(jnp.float32)).reshape(blk // 8, 8, HEAD), axis=0))
                pos += blk
        flag[0] = jnp.where(jnp.logical_and(jnp.max(vmax) < SAFE_VALUE, bound_ref[0] < SAFE_SCORE), 1, 0)

    q = qt[b]

    def write(val):
        @pl.when(b == 0)
        def _():
            tout[...] = val
        for s in range(n_src):
            for c in range(rows // blk):
                @pl.when(b == 1 + s * (rows // blk) + c)
                def _():
                    outs[s][pl.ds(c * blk, blk), :] = val

    @pl.when(flag[0] == 1)
    def _():
        acc = jnp.zeros((HEAD, blk), jnp.float32)
        tot = jnp.zeros((8, blk), jnp.float32)
        for i in range(keys // kb):
            s = jnp.dot(ks[pl.ds(i * kb, kb), :], q, preferred_element_type=jnp.float32)
            p = jnp.exp2(s * scale2)
            tot = tot + jnp.sum(p.reshape(kb // 8, 8, blk), axis=0)
            acc = acc + jnp.dot(vt[:, pl.ds(i * kb, kb)], p.astype(jnp.bfloat16), preferred_element_type=jnp.float32)
        total = jnp.sum(tot, axis=0, keepdims=True)
        write((acc / total).T.astype(jnp.bfloat16))

    @pl.when(flag[0] == 0)
    def _():
        def body(i, carry):
            acc, tot, peak = carry
            st = pl.multiple_of(i * blk, blk)
            s = jnp.dot(ks[pl.ds(st, blk), :], q, preferred_element_type=jnp.float32) * scale2
            new = jnp.maximum(peak, jnp.max(s, axis=0, keepdims=True))
            p = jnp.exp2(s - new)
            factor = jnp.exp2(peak - new)
            tot = tot * factor + jnp.sum(p, axis=0, keepdims=True)
            acc = acc * factor + jnp.dot(vt[:, pl.ds(st, blk)], p.astype(jnp.bfloat16), preferred_element_type=jnp.float32)
            return acc, tot, new
        start = (jnp.zeros((HEAD, blk), jnp.float32), jnp.zeros((1, blk), jnp.float32), jnp.full((1, blk), -jnp.inf, jnp.float32))
        acc, tot, _ = lax.fori_loop(0, keys // blk, body, start)
        write((acc / tot).T.astype(jnp.bfloat16))


def attend(bound, srcs, text, blk=512, kb=4352):
    n_src, rows, txt = len(srcs), srcs[0].shape[1], text.shape[1]
    keys = n_src * rows + txt
    return pl.pallas_call(
        functools.partial(attend_kernel, n_src=n_src, blk=blk, kb=kb),
        out_shape=[jax.ShapeDtypeStruct((rows, HEAD), jnp.bfloat16)] * n_src + [jax.ShapeDtypeStruct((txt, HEAD), jnp.bfloat16)],
        grid_spec=pltpu.PrefetchScalarGridSpec(
            num_scalar_prefetch=1, grid=(keys // blk,),
            in_specs=[whole_block((3, rows, HEAD))] * n_src + [whole_block((3, txt, HEAD))],
            out_specs=[whole_block((rows, HEAD))] * n_src + [whole_block((txt, HEAD))],
            scratch_shapes=[pltpu.VMEM((keys // blk, HEAD, blk), jnp.bfloat16), pltpu.VMEM((keys, HEAD), jnp.bfloat16),
                            pltpu.VMEM((HEAD, keys), jnp.bfloat16), pltpu.SMEM((1,), jnp.int32)]),
        compiler_params=params(1), cost_estimate=cost(4 * keys * keys * HEAD, 8 * keys * HEAD, keys * keys),
        name="attend",
    )(bound, *srcs, text)


def image_out_kernel(me_ref, *refs, heads, tile):
    o_refs, w_refs = refs[:heads], refs[heads:2 * heads]
    x_ref, gate_ref, b_ref, r_ref = refs[2 * heads:]
    weights = jnp.concatenate([w[0] for w in w_refs], axis=0)
    for m in range(x_ref.shape[0] // tile):
        sl = pl.ds(m * tile, tile)
        rows = jnp.concatenate([o[sl, :] for o in o_refs], axis=1)
        acc = jnp.dot(rows, weights, preferred_element_type=jnp.float32)
        r_ref[sl, :] = x_ref[sl, :].astype(jnp.float32) + gate_ref[...] * (acc + b_ref[...])


def image_out(me, attended, w_out, x, gate, bias, group):
    rows, hidden = x.shape
    heads = len(attended)
    step = 512

    def row(h):
        return lambda n, me: (0, (h // group) * group + jnp.bitwise_xor(me[0], h % group), n)

    return pl.pallas_call(
        functools.partial(image_out_kernel, heads=heads, tile=256),
        out_shape=jax.ShapeDtypeStruct((rows, hidden), jnp.float32),
        grid_spec=pltpu.PrefetchScalarGridSpec(
            num_scalar_prefetch=1, grid=(hidden // step,),
            in_specs=[whole_block((rows, HEAD))] * heads + [pl.BlockSpec((1, HEAD, step), row(h)) for h in range(heads)]
            + [pl.BlockSpec((rows, step), lambda n, me: (0, n)), pl.BlockSpec((1, step), lambda n, me: (0, n)),
               pl.BlockSpec((1, step), lambda n, me: (0, n))],
            out_specs=pl.BlockSpec((rows, step), lambda n, me: (0, n))),
        compiler_params=params(1), cost_estimate=cost(2 * rows * hidden * hidden, 2 * hidden * hidden + 8 * rows * hidden),
        name="image_out",
    )(me, *attended, *([w_out] * heads), x, gate, bias)


def text_up_kernel(me_ref, h_ref, w_ref, b_ref, u_ref):
    acc = jnp.dot(h_ref[...], w_ref[0], preferred_element_type=jnp.float32) + b_ref[0]
    u_ref[...] = jax.nn.gelu(acc, approximate=True).astype(jnp.bfloat16)


def text_down_kernel(me_ref, u_ref, w_ref, out_ref):
    out_ref[...] = jnp.dot(u_ref[...], w_ref[0], preferred_element_type=jnp.float32)


def text_ff(me, h, w_up, b_up, w_down, group):
    rows, hidden = h.shape
    share = w_up.shape[2] // group
    step = 512
    n_up = share // step
    inner = pl.pallas_call(
        text_up_kernel,
        out_shape=jax.ShapeDtypeStruct((rows, share), jnp.bfloat16),
        grid_spec=pltpu.PrefetchScalarGridSpec(
            num_scalar_prefetch=1, grid=(n_up,),
            in_specs=[whole_block((rows, hidden)), pl.BlockSpec((1, hidden, step), lambda n, me: (1, 0, me[0] * n_up + n)),
                      pl.BlockSpec((1, 1, step), lambda n, me: (1, 0, me[0] * n_up + n))],
            out_specs=pl.BlockSpec((rows, step), lambda n, me: (0, n))),
        compiler_params=params(1), cost_estimate=cost(2 * rows * hidden * share, 2 * hidden * share), name="text_up",
    )(me, h, w_up, b_up)
    return pl.pallas_call(
        text_down_kernel,
        out_shape=jax.ShapeDtypeStruct((rows, hidden), jnp.float32),
        grid_spec=pltpu.PrefetchScalarGridSpec(
            num_scalar_prefetch=1, grid=(hidden // step,),
            in_specs=[whole_block((rows, share)), pl.BlockSpec((1, share, step), lambda n, me: (1, me[0], n))],
            out_specs=pl.BlockSpec((rows, step), lambda n, me: (0, n))),
        compiler_params=params(1), cost_estimate=cost(2 * rows * hidden * share, 2 * hidden * share), name="text_down",
    )(me, inner, w_down)


def solution(mesh):
    group = mesh.shape['cp']

    def local(image, text, cond_vec, rope_cos, rope_sin, w_mod, b_mod, w_qkv, b_qkv, qk_gain, w_out, b_out, w_up, b_up, w_down, b_down):
        hidden = image.shape[-1]
        heads = hidden // HEAD
        slots = heads // group
        me = jnp.reshape(lax.axis_index('cp'), (1,)).astype(jnp.int32)

        activated = jax.nn.silu(cond_vec.astype(jnp.float32)).astype(jnp.bfloat16)
        columns = mod_columns(me, jnp.broadcast_to(activated, (16, hidden)), w_mod, group)[:, 0, :]
        mod = lax.all_gather(columns, 'cp', axis=1, tiled=True) + b_mod
        mod = mod.reshape(2, 6, 1, hidden)

        b_qkv3 = b_qkv.reshape(2, 1, -1)
        b_up3 = b_up.reshape(2, 1, -1)
        gains = qk_gain.reshape(2, 2, 1, HEAD)
        cos = jnp.concatenate([rope_cos, rope_cos], axis=1)
        sin = jnp.concatenate([-rope_sin, rope_sin], axis=1)
        peaks = jnp.max(jnp.abs(qk_gain), axis=(0, 2))
        bound = jnp.reshape(1.02 * HEAD ** 0.5 * peaks[0] * peaks[1], (1,))

        h_img = (layer_norm(image.astype(jnp.float32)) * (1.0 + mod[0, 1]) + mod[0, 0]).astype(jnp.bfloat16)
        h_txt = (layer_norm(text.astype(jnp.float32)) * (1.0 + mod[1, 1]) + mod[1, 0]).astype(jnp.bfloat16)

        def swap(value, bits):
            return lax.ppermute(value, 'cp', [(i, i ^ bits) for i in range(group)])

        arrived = []
        for j in range(slots):
            pieces = image_qkv(me, h_img, w_qkv, b_qkv3, gains[0], cos, sin, j, group)
            arrived.append([pieces[0]] + [swap(pieces[s], s) for s in range(1, group)])
        t_qkv = text_qkv(me, h_txt, w_qkv, b_qkv3, gains[1], slots, group)

        attended, t_att = [], []
        for j in range(slots):
            res = attend(bound, arrived[j], t_qkv[j])
            attended.extend([res[0]] + [swap(res[s], s) for s in range(1, group)])
            t_att.append(res[group])

        t_all = lax.all_gather(jnp.stack(t_att), 'cp', axis=0, tiled=False)
        t_all = jnp.transpose(t_all, (2, 1, 0, 3)).reshape(text.shape[0], hidden)
        t_res = text.astype(jnp.float32) + mod[1, 2] * (jnp.dot(t_all, w_out[1], preferred_element_type=jnp.float32) + b_out[1])
        t_normed = (layer_norm(t_res) * (1.0 + mod[1, 4]) + mod[1, 3]).astype(jnp.bfloat16)
        t_part = text_ff(me, t_normed, w_up, b_up3, w_down, group)
        t_sum = lax.psum(t_part, 'cp')
        text_out = (t_res + mod[1, 5] * (t_sum + b_down[1])).astype(jnp.bfloat16)

        res = image_out(me, attended, w_out, image, mod[0, 2], b_out[0][None], group)
        normed = (layer_norm(res) * (1.0 + mod[0, 4]) + mod[0, 3]).astype(jnp.bfloat16)
        inner = jax.nn.gelu(jnp.dot(normed, w_up[0], preferred_element_type=jnp.float32) + b_up[0], approximate=True).astype(jnp.bfloat16)
        image_out_rows = (res + mod[0, 5] * (jnp.dot(inner, w_down[0], preferred_element_type=jnp.float32) + b_down[0])).astype(jnp.bfloat16)
        return image_out_rows, text_out

    rows_spec = P(('dp', 'cp'), None)
    text_spec = P('dp', None)
    whole = P()
    return jax.shard_map(local, mesh=mesh,
                         in_specs=(rows_spec, text_spec, text_spec, rows_spec, rows_spec) + (whole,) * 11,
                         out_specs=(rows_spec, text_spec), check_vma=False)
```

```python
import functools

import jax
import jax.numpy as jnp
from jax import lax
from jax.experimental import pallas as pl
from jax.experimental.pallas import tpu as pltpu
from jax.sharding import PartitionSpec as P

NORM_EPS = 1e-6
HEAD = 128
LOG2E = 1.4426950408889634
SAFE_SCORE = 60.0
SAFE_POWER = 26.0
MESH = pl.DeviceIdType.MESH


def params(dims):
    return pltpu.CompilerParams(dimension_semantics=("arbitrary",) * dims, vmem_limit_bytes=60 * 2**20)


def cost(flops, moved, trans=0):
    return pl.CostEstimate(flops=flops, bytes_accessed=moved, transcendentals=trans)


def whole_block(shape):
    return pl.BlockSpec(shape, lambda *_: (0,) * len(shape))


def layer_norm(rows):
    mean = jnp.mean(rows, axis=-1, keepdims=True)
    centered = rows - mean
    return centered * lax.rsqrt(jnp.mean(centered * centered, axis=-1, keepdims=True) + NORM_EPS)


def mod_kernel(me_ref, act_ref, w_ref, out_ref):
    out_ref[0] = jnp.dot(act_ref[...], w_ref[0], preferred_element_type=jnp.float32)


def mod_columns(me, activated, w_mod, group):
    branches, hidden, width = w_mod.shape
    share = width // group
    step = share // 3
    rows = activated.shape[0]
    return pl.pallas_call(
        mod_kernel,
        out_shape=jax.ShapeDtypeStruct((branches, rows, share), jnp.float32),
        grid_spec=pltpu.PrefetchScalarGridSpec(
            num_scalar_prefetch=1, grid=(branches, 3),
            in_specs=[whole_block((rows, hidden)),
                      pl.BlockSpec((1, hidden, step), lambda b, n, me: (b, 0, me[0] * 3 + n))],
            out_specs=pl.BlockSpec((1, rows, step), lambda b, n, me: (b, 0, n))),
        compiler_params=params(2), cost_estimate=cost(2 * branches * rows * hidden * share, 2 * branches * hidden * share),
        name="modulate",
    )(me, activated, w_mod)


def head_norm(t, gain):
    x = t.astype(jnp.bfloat16).astype(jnp.float32)
    return x * lax.rsqrt(jnp.mean(x * x, axis=-1, keepdims=True) + NORM_EPS) * gain


def image_qkv_kernel(me_ref, h_ref, *refs, per, tile):
    w_refs, b_refs = refs[:per], refs[per:2 * per]
    gain_ref, cos_ref, sin_ref = refs[2 * per:2 * per + 3]
    outs = refs[2 * per + 3:]
    half, t = pl.program_id(0), pl.program_id(1)
    rows = h_ref.shape[0]

    def run(kind, group):
        weights = jnp.concatenate([w[0] for w in w_refs], axis=1)
        bias = jnp.concatenate([b[0] for b in b_refs], axis=1)
        for m in range(rows // tile):
            sl = pl.ds(m * tile, tile)
            acc = jnp.dot(h_ref[sl, :], weights, preferred_element_type=jnp.float32) + bias
            for i in range(per):
                piece = acc[:, i * HEAD:(i + 1) * HEAD]
                if kind == "v":
                    res = piece
                else:
                    y = head_norm(piece, gain_ref[0])
                    res = y * cos_ref[sl, :] + pltpu.roll(y, HEAD // 2, 1) * sin_ref[sl, :]
                outs[group * per + i][0, sl, :] = res.astype(jnp.bfloat16)

    for group in range(len(outs) // per):
        @pl.when(jnp.logical_and(half == group, t < 2))
        def _():
            run("qk", group)

        @pl.when(jnp.logical_and(half == group, t == 2))
        def _():
            run("v", group)


def image_qkv(me, h, w_qkv, b_qkv, gains, cos, sin, slot, group):
    rows, hidden = h.shape
    heads = hidden // HEAD
    per = 4
    halves = group // per

    def col(i):
        return lambda half, t, me: (0, 0, t * heads + slot * group + jnp.bitwise_xor(me[0], half * per + i))

    def out_map(own):
        def index(half, t, me):
            return (jnp.where(half < own, 0, jnp.where(half == own, t, 2)), 0, 0)
        return index

    return pl.pallas_call(
        functools.partial(image_qkv_kernel, per=per, tile=256),
        out_shape=[jax.ShapeDtypeStruct((3, rows, HEAD), jnp.bfloat16)] * group,
        grid_spec=pltpu.PrefetchScalarGridSpec(
            num_scalar_prefetch=1, grid=(halves, 3),
            in_specs=[whole_block((rows, hidden))]
            + [pl.BlockSpec((1, hidden, HEAD), col(i)) for i in range(per)]
            + [pl.BlockSpec((1, 1, HEAD), col(i)) for i in range(per)]
            + [pl.BlockSpec((1, 1, HEAD), lambda half, t, me: (jnp.minimum(t, 1), 0, 0)),
               whole_block((rows, HEAD)), whole_block((rows, HEAD))],
            out_specs=[pl.BlockSpec((1, rows, HEAD), out_map(s // per)) for s in range(group)]),
        compiler_params=params(2), cost_estimate=cost(2 * rows * hidden * 3 * group * HEAD, 2 * hidden * 3 * group * HEAD),
        name="image_qkv",
    )(me, h, *([w_qkv] * per), *([b_qkv] * per), gains, cos, sin)


def text_qkv_kernel(me_ref, h_ref, w_ref, b_ref, gain_ref, out_ref):
    t = pl.program_id(1)
    acc = jnp.dot(h_ref[...], w_ref[0], preferred_element_type=jnp.float32) + b_ref[0]
    normed = head_norm(acc, gain_ref[0])
    out_ref[0, 0] = jnp.where(t < 2, normed, acc).astype(jnp.bfloat16)


def text_qkv(me, h, w_qkv, b_qkv, gains, slots, group):
    rows, hidden = h.shape
    heads = hidden // HEAD

    def col(j, t, me):
        return (1, 0, t * heads + j * group + me[0])

    return pl.pallas_call(
        text_qkv_kernel,
        out_shape=jax.ShapeDtypeStruct((slots, 3, rows, HEAD), jnp.bfloat16),
        grid_spec=pltpu.PrefetchScalarGridSpec(
            num_scalar_prefetch=1, grid=(slots, 3),
            in_specs=[whole_block((rows, hidden)), pl.BlockSpec((1, hidden, HEAD), col), pl.BlockSpec((1, 1, HEAD), col),
                      pl.BlockSpec((1, 1, HEAD), lambda j, t, me: (jnp.minimum(t, 1), 0, 0))],
            out_specs=pl.BlockSpec((1, 1, rows, HEAD), lambda j, t, me: (j, t, 0, 0))),
        compiler_params=params(2), cost_estimate=cost(2 * rows * hidden * 3 * slots * HEAD, 2 * hidden * 3 * slots * HEAD),
        name="text_qkv",
    )(me, h, w_qkv, b_qkv, gains)


def flip(me, s):
    total = 0
    for k in (1, 2, 4):
        x, y = lax.rem(lax.div(me, k), 2), lax.rem(lax.div(s, k), 2)
        total = total + k * (x + y - 2 * x * y)
    return total


def exchange_kernel(*refs, slots, group, blk, kb):
    first, rest = refs[:group], refs[group:]
    later = [rest[j * group:(j + 1) * group] for j in range(slots - 1)]
    (text, o_recv, t_recv, held, qt, ks, vt, stage, obuf, unscale,
     in_sems, qkv_send, qkv_recv, o_send, o_arrive, t_send, t_arrive) = rest[(slots - 1) * group:]
    i = pl.program_id(0)
    me = lax.axis_index('cp')
    keys = ks.shape[0]
    rows, txt = first[0].shape[1], text.shape[2]
    halves = rows // blk
    n_blocks = keys // blk
    scale2 = LOG2E * HEAD ** -0.5

    def peer(s):
        return {'cp': flip(me, s)}

    def send_rows(j, s):
        return pltpu.make_async_remote_copy(src_ref=later[j - 1][s], dst_ref=held.at[j - 1, s], send_sem=qkv_send.at[j - 1, s],
                                            recv_sem=qkv_recv.at[j - 1, s], device_id=peer(s), device_id_type=MESH)

    def text_copy(slot, j, s):
        if s == 0:
            return pltpu.make_async_copy(obuf.at[slot], t_recv.at[j, 0], t_send.at[j, 0])
        return pltpu.make_async_remote_copy(src_ref=obuf.at[slot], dst_ref=t_recv.at[j, s], send_sem=t_send.at[j, s],
                                            recv_sem=t_arrive.at[j, s], device_id=peer(s), device_id_type=MESH)

    def hand_on(j, s):
        return pltpu.make_async_remote_copy(src_ref=t_recv.at[j, s], dst_ref=t_recv.at[j, s + 1], send_sem=t_send.at[j, s + 1],
                                            recv_sem=t_arrive.at[j, s + 1], device_id=peer(1), device_id_type=MESH)

    def relay(j):
        for s in range(2, group, 2):
            text_copy(0, j, s).wait_recv()
            hand_on(j, s).start()

    def far_copy(slot, j, s, half):
        return pltpu.make_async_remote_copy(src_ref=obuf.at[slot], dst_ref=o_recv.at[j, s, pl.ds(half * blk, blk)],
                                            send_sem=o_send.at[j, s, half], recv_sem=o_arrive.at[j, s, half],
                                            device_id=peer(s), device_id_type=MESH)

    def near_copy(slot, j, half):
        return pltpu.make_async_copy(obuf.at[slot], o_recv.at[j, 0, pl.ds(half * blk, blk)], o_send.at[j, 0, half])

    def send_block(n):
        j, b = lax.div(n, n_blocks), lax.rem(n, n_blocks)
        s = group - 1 - lax.div(b - 1, halves)
        half = lax.rem(b - 1 + halves, halves)

        @pl.when(b == 0)
        def _():
            for t in (0, 1) + tuple(range(2, group, 2)):
                text_copy(n, j, t).start()

        @pl.when(jnp.logical_and(b > 0, b <= (group - 1) * halves))
        def _():
            far_copy(n, j, s, half).start()

        @pl.when(b > (group - 1) * halves)
        def _():
            near_copy(n, j, half).start()

    @pl.when(i == 0)
    def _():
        barrier = pltpu.get_barrier_semaphore()
        for s in range(1, group):
            pl.semaphore_signal(barrier, inc=1, device_id=peer(s), device_id_type=MESH)
        pl.semaphore_wait(barrier, group - 1)
        for j in range(1, slots):
            for s in range(group - 1, 0, -1):
                send_rows(j, s).start()

    @pl.when(i > 0)
    def _():
        send_block(i - 1)

    @pl.when(i == slots * n_blocks - 3)
    def _():
        for j in range(slots - 1):
            relay(j)

    def prepare(j):
        order = [(group - 1 - p) for p in range(group)]
        loads = []
        pos = txt
        for p, s in enumerate(order):
            if j == 0:
                source = first[s]
            elif s == 0:
                source = later[j - 1][0]
            else:
                send_rows(j, s).wait_recv()
                source = held.at[j - 1, s]
            for t in range(3):
                target = ks.at[pl.ds(pos, rows)] if t == 1 else stage.at[p, t // 2]
                copy = pltpu.make_async_copy(source.at[t], target, in_sems.at[p, t])
                copy.start()
                loads.append(copy)
            pos += rows
        qt[0] = text[j, 0].T
        ks[pl.ds(0, txt), :] = text[j, 1]
        for copy in loads:
            copy.wait()
        tv = text[j, 2].astype(jnp.float32)
        top = jnp.max(jnp.abs(tv).reshape(txt // 8, 8, HEAD), axis=0)
        for p in range(group):
            top = jnp.maximum(top, jnp.max(jnp.abs(stage[p, 1].astype(jnp.float32)).reshape(rows // 8, 8, HEAD), axis=0))
        top = jnp.max(jnp.max(top, axis=0, keepdims=True), axis=1, keepdims=True)
        power = jnp.maximum(jnp.ceil(jnp.log2(jnp.maximum(top, 1.0))) - SAFE_POWER, 0.0)
        shrink = jnp.exp2(-power)
        unscale[...] = jnp.broadcast_to(jnp.exp2(power), unscale.shape)
        vt[:, pl.ds(0, txt)] = (tv * shrink).astype(jnp.bfloat16).T
        for p in range(group):
            for c in range(halves):
                sl = pl.ds(c * blk, blk)
                qt[1 + p * halves + c] = stage[p, 0, sl, :].T
                v = (stage[p, 1, sl, :].astype(jnp.float32) * shrink).astype(jnp.bfloat16)
                vt[:, pl.ds(txt + p * rows + c * blk, blk)] = v.T

    for j in range(slots):
        @pl.when(i == j * n_blocks)
        def _():
            prepare(j)

    q = qt[lax.rem(i, n_blocks)]
    acc = jnp.zeros((HEAD, blk), jnp.float32)
    tot = jnp.zeros((8, blk), jnp.float32)
    for c in range(keys // kb):
        sc = jnp.dot(ks[pl.ds(c * kb, kb), :], q, preferred_element_type=jnp.float32)
        p = jnp.exp2(sc * scale2)
        tot = tot + jnp.sum(p.reshape(kb // 8, 8, blk), axis=0)
        acc = acc + jnp.dot(vt[:, pl.ds(c * kb, kb)], p.astype(jnp.bfloat16), preferred_element_type=jnp.float32)
    total = jnp.sum(tot, axis=0, keepdims=True)
    obuf[i] = (acc / total * unscale[0:1, 0:1]).T.astype(jnp.bfloat16)

    @pl.when(i == slots * n_blocks - 1)
    def _():
        send_block(i)
        relay(slots - 1)
        for j in range(slots):
            text_copy(0, j, 0).wait()
            text_copy(0, j, 1).wait()
            for s in range(2, group, 2):
                text_copy(0, j, s).wait_send()
                hand_on(j, s).wait()
            for half in range(halves):
                near_copy(0, j, half).wait()
            for s in range(1, group):
                if j > 0:
                    send_rows(j, s).wait_send()
                for half in range(halves):
                    far_copy(0, j, s, half).wait()


def exchange_attend(first, later, text, blk=512, kb=4352):
    group, slots = len(first), 1 + len(later)
    rows, txt = first[0].shape[1], text.shape[2]
    keys = group * rows + txt
    any_space = pl.BlockSpec(memory_space=pl.ANY)
    dma = pltpu.SemaphoreType.DMA
    bf16 = jnp.bfloat16
    o_recv, t_recv, _ = pl.pallas_call(
        functools.partial(exchange_kernel, slots=slots, group=group, blk=blk, kb=kb),
        out_shape=[jax.ShapeDtypeStruct((slots, group, rows, HEAD), bf16), jax.ShapeDtypeStruct((slots, group, txt, HEAD), bf16),
                   jax.ShapeDtypeStruct((slots - 1, group, 3, rows, HEAD), bf16)],
        grid=(slots * (keys // blk),),
        in_specs=[any_space] * (group * slots) + [whole_block(text.shape)],
        out_specs=[any_space] * 3,
        scratch_shapes=[pltpu.VMEM((keys // blk, HEAD, blk), bf16), pltpu.VMEM((keys, HEAD), bf16), pltpu.VMEM((HEAD, keys), bf16),
                        pltpu.VMEM((group, 2, rows, HEAD), bf16), pltpu.VMEM((slots * (keys // blk), blk, HEAD), bf16), pltpu.VMEM((8, HEAD), jnp.float32),
                        dma((group, 3)), dma((slots - 1, group)), dma((slots - 1, group)),
                        dma((slots, group, rows // blk)), dma((slots, group, rows // blk)), dma((slots, group)), dma((slots, group))],
        compiler_params=pltpu.CompilerParams(dimension_semantics=("arbitrary",), vmem_limit_bytes=60 * 2**20,
                                             collective_id=0, has_side_effects=True),
        cost_estimate=cost(slots * 4 * keys * keys * HEAD, slots * 8 * keys * HEAD, slots * keys * keys),
        name="exchange_attend",
    )(*first, *[piece for pieces in later for piece in pieces], text)
    return o_recv, t_recv


def attend_kernel(*refs, n_src, blk):
    srcs, tref = refs[:n_src], refs[n_src]
    o_ref, tout = refs[n_src + 1:n_src + 3]
    qt, ks, vt = refs[n_src + 3:]
    b = pl.program_id(0)
    keys = ks.shape[0]
    rows, txt = srcs[0].shape[1], tref.shape[1]
    scale2 = LOG2E * HEAD ** -0.5

    @pl.when(b == 0)
    def _():
        pos = 0
        for ref in (tref,) + tuple(srcs):
            for c in range(ref.shape[1] // blk):
                sl = pl.ds(c * blk, blk)
                qt[pos // blk] = ref[0, sl, :].T
                ks[pl.ds(pos, blk), :] = ref[1, sl, :]
                vt[:, pl.ds(pos, blk)] = ref[2, sl, :].T
                pos += blk

    q = qt[b]

    def body(i, carry):
        acc, tot, peak = carry
        st = pl.multiple_of(i * blk, blk)
        sc = jnp.dot(ks[pl.ds(st, blk), :], q, preferred_element_type=jnp.float32) * scale2
        new = jnp.maximum(peak, jnp.max(sc, axis=0, keepdims=True))
        p = jnp.exp2(sc - new)
        factor = jnp.exp2(peak - new)
        tot = tot * factor + jnp.sum(p, axis=0, keepdims=True)
        acc = acc * factor + jnp.dot(vt[:, pl.ds(st, blk)], p.astype(jnp.bfloat16), preferred_element_type=jnp.float32)
        return acc, tot, new

    start = (jnp.zeros((HEAD, blk), jnp.float32), jnp.zeros((1, blk), jnp.float32), jnp.full((1, blk), -jnp.inf, jnp.float32))
    acc, tot, _ = lax.fori_loop(0, keys // blk, body, start)
    val = (acc / tot).T.astype(jnp.bfloat16)

    @pl.when(b == 0)
    def _():
        tout[...] = val

    @pl.when(b > 0)
    def _():
        o_ref[pl.ds(pl.multiple_of((b - 1) * blk, blk), blk), :] = val


def attend(srcs, text, blk=512):
    n_src, rows, txt = len(srcs), srcs[0].shape[1], text.shape[1]
    keys = n_src * rows + txt
    return pl.pallas_call(
        functools.partial(attend_kernel, n_src=n_src, blk=blk),
        out_shape=[jax.ShapeDtypeStruct((n_src * rows, HEAD), jnp.bfloat16), jax.ShapeDtypeStruct((txt, HEAD), jnp.bfloat16)],
        grid=(keys // blk,),
        in_specs=[whole_block((3, rows, HEAD))] * n_src + [whole_block((3, txt, HEAD))],
        out_specs=[whole_block((n_src * rows, HEAD)), whole_block((txt, HEAD))],
        scratch_shapes=[pltpu.VMEM((keys // blk, HEAD, blk), jnp.bfloat16), pltpu.VMEM((keys, HEAD), jnp.bfloat16),
                        pltpu.VMEM((HEAD, keys), jnp.bfloat16)],
        compiler_params=params(1), cost_estimate=cost(4 * keys * keys * HEAD, 8 * keys * HEAD, keys * keys), name="attend",
    )(*srcs, text)


def norm_kernel(x_ref, shift_ref, scale_ref, out_ref):
    out_ref[...] = (layer_norm(x_ref[...].astype(jnp.float32)) * (1.0 + scale_ref[...]) + shift_ref[...]).astype(jnp.bfloat16)


def modulated_norm(x, shift, scale):
    rows, hidden = x.shape
    block = pl.BlockSpec((128, hidden), lambda i: (i, 0))
    return pl.pallas_call(
        norm_kernel, out_shape=jax.ShapeDtypeStruct(x.shape, jnp.bfloat16), grid=(rows // 128,),
        in_specs=[block, whole_block((1, hidden)), whole_block((1, hidden))], out_specs=block,
        compiler_params=params(1), cost_estimate=cost(10 * rows * hidden, 4 * rows * hidden), name="norm",
    )(x, shift, scale)


def finish_kernel(me_ref, *refs, n_o, heads, n_proj, n_ff, step, tile, place, split):
    o_refs = refs[:n_o]
    x_ref, w_out, w_up, w_down, mod_ref, b_out, b_up, b_down = refs[n_o:n_o + 8]
    if split:
        part_ref, r_out, rows_buf, r_ref, in_sems, out_sems = refs[n_o + 8:]
    else:
        y_out, rows_buf, r_ref, in_sems, out_sems = refs[n_o + 8:]
    i = pl.program_id(0)
    rows = r_ref.shape[0]
    tiles = [pl.ds(m * tile, tile) for m in range(rows // tile)]

    def fetch(h):
        spot = pl.multiple_of(place(h, me_ref[0]) * HEAD, HEAD)
        source = o_refs[h] if n_o > 1 else o_refs[0].at[h]
        return pltpu.make_async_copy(source, rows_buf.at[:, pl.ds(spot, HEAD)], in_sems.at[h])

    @pl.when(i == 0)
    def _():
        for h in range(heads):
            fetch(h).start()
        for h in range(heads):
            fetch(h).wait()

    @pl.when(i < n_proj)
    def _():
        cols = pl.ds(pl.multiple_of(i * step, step), step)
        for sl in tiles:
            acc = jnp.dot(rows_buf[sl, :], w_out[0], preferred_element_type=jnp.float32)
            r_ref[sl, cols] = x_ref[sl, :].astype(jnp.float32) + mod_ref[2, :, cols] * (acc + b_out[:, cols])

    def r_copy():
        return pltpu.make_async_copy(r_ref, r_out, out_sems.at[0])

    def y_copy(m):
        return pltpu.make_async_copy(rows_buf.at[tiles[m]], y_out.at[tiles[m]], out_sems.at[m])

    def feed(first, last):
        if split and first:
            r_copy().start()
        for m, sl in enumerate(tiles):
            if first:
                res = r_ref[sl, :]
                h = (layer_norm(res) * (1.0 + mod_ref[4]) + mod_ref[3]).astype(jnp.bfloat16)
                rows_buf[sl, :] = h
            else:
                h = rows_buf[sl, :]
            u = jnp.dot(h, w_up[0], preferred_element_type=jnp.float32) + b_up[0]
            u = jax.nn.gelu(u, approximate=True).astype(jnp.bfloat16)
            part = jnp.dot(u, w_down[0], preferred_element_type=jnp.float32)
            if split:
                part_ref[sl, :] = part if first else part_ref[sl, :] + part
                continue
            base = res + mod_ref[5] * b_down[...] if first else r_ref[sl, :]
            total = base + mod_ref[5] * part
            if last:
                rows_buf[sl, :] = total.astype(jnp.bfloat16)
                y_copy(m).start()
            else:
                r_ref[sl, :] = total
        if last:
            if split:
                r_copy().wait()
            else:
                for m in range(len(tiles)):
                    y_copy(m).wait()

    final = n_proj + n_ff - 1

    @pl.when(i == n_proj)
    def _():
        feed(True, False)

    @pl.when(jnp.logical_and(i > n_proj, i < final))
    def _():
        feed(False, False)

    @pl.when(i == final)
    def _():
        feed(False, True)


def finish(me, attended, place, x, mod, w_out, b_out, w_up, b_up, w_down, b_down, branch, share, split):
    rows, hidden = x.shape
    step, tile = 512, min(rows, 1024)
    n_proj, n_ff = hidden // step, share // step
    n_o, heads = len(attended), hidden // HEAD

    def proj(i):
        return jnp.minimum(i, n_proj - 1)

    def ff(i, me):
        at = jnp.clip(i - n_proj, 0, n_ff - 1)
        return at + me[0] * n_ff if split else at

    any_space = pl.BlockSpec(memory_space=pl.ANY)
    if split:
        out_shape = [jax.ShapeDtypeStruct((rows, hidden), jnp.float32)] * 2
        out_specs = [whole_block((rows, hidden)), any_space]
    else:
        out_shape = jax.ShapeDtypeStruct((rows, hidden), jnp.bfloat16)
        out_specs = any_space
    return pl.pallas_call(
        functools.partial(finish_kernel, n_o=n_o, heads=heads, n_proj=n_proj, n_ff=n_ff, step=step, tile=tile, place=place, split=split),
        out_shape=out_shape,
        grid_spec=pltpu.PrefetchScalarGridSpec(
            num_scalar_prefetch=1, grid=(n_proj + n_ff,),
            in_specs=[any_space] * n_o
            + [pl.BlockSpec((rows, step), lambda i, me: (0, proj(i))),
               pl.BlockSpec((1, hidden, step), lambda i, me: (branch, 0, proj(i))),
               pl.BlockSpec((1, hidden, step), lambda i, me: (branch, 0, ff(i, me))),
               pl.BlockSpec((1, step, hidden), lambda i, me: (branch, ff(i, me), 0)),
               whole_block((6, 1, hidden)), whole_block((1, hidden)),
               pl.BlockSpec((1, 1, step), lambda i, me: (branch, 0, ff(i, me))), whole_block((1, hidden))],
            out_specs=out_specs,
            scratch_shapes=[pltpu.VMEM((rows, hidden), jnp.bfloat16), pltpu.VMEM((rows, hidden), jnp.float32),
                            pltpu.SemaphoreType.DMA((heads,)), pltpu.SemaphoreType.DMA((rows // tile,))]),
        compiler_params=params(1),
        cost_estimate=cost(2 * rows * hidden * (hidden + 2 * share), 2 * hidden * (hidden + 2 * share) + 8 * rows * hidden),
        name="finish_text" if split else "finish_image",
    )(me, *attended, x, w_out, w_up, w_down, mod, b_out, b_up, b_down)


def solution(mesh):
    group = mesh.shape['cp']

    def local(image, text, cond_vec, rope_cos, rope_sin, w_mod, b_mod, w_qkv, b_qkv, qk_gain, w_out, b_out, w_up, b_up, w_down, b_down):
        hidden = image.shape[-1]
        heads = hidden // HEAD
        slots = heads // group
        me = jnp.reshape(lax.axis_index('cp'), (1,)).astype(jnp.int32)

        activated = jax.nn.silu(cond_vec.astype(jnp.float32)).astype(jnp.bfloat16)
        columns = mod_columns(me, jnp.broadcast_to(activated, (16, hidden)), w_mod, group)[:, 0, :]
        mod = lax.all_gather(columns, 'cp', axis=1, tiled=True) + b_mod
        mod = mod.reshape(2, 6, 1, hidden)

        b_qkv3 = b_qkv.reshape(2, 1, -1)
        b_up3 = b_up.reshape(2, 1, -1)
        gains = qk_gain.reshape(2, 2, 1, HEAD)
        cos = jnp.concatenate([rope_cos, rope_cos], axis=1)
        sin = jnp.concatenate([-rope_sin, rope_sin], axis=1)
        peaks = jnp.max(jnp.abs(qk_gain), axis=(0, 2))
        bound = 1.02 * HEAD ** 0.5 * peaks[0] * peaks[1]

        h_img = modulated_norm(image, mod[0, 0], mod[0, 1])
        h_txt = modulated_norm(text, mod[1, 0], mod[1, 1])

        def swap(value, bits):
            return lax.ppermute(value, 'cp', [(i, i ^ bits) for i in range(group)])

        pieces = [image_qkv(me, h_img, w_qkv, b_qkv3, gains[0], cos, sin, j, group) for j in range(slots)]
        first = [pieces[0][0]] + [swap(pieces[0][s], s) for s in range(1, group)]
        t_qkv = text_qkv(me, h_txt, w_qkv, b_qkv3, gains[1], slots, group)

        def bounded(first, later, t_qkv):
            return exchange_attend(first, later, t_qkv)

        def general(first, later, t_qkv):
            o_all, t_all = [], []
            for j in range(slots):
                srcs = first if j == 0 else [later[j - 1][0]] + [swap(later[j - 1][s], s) for s in range(1, group)]
                o, t = attend(srcs, t_qkv[j])
                o = o.reshape(group, -1, HEAD)
                o_all.append(jnp.stack([o[0]] + [swap(o[s], s) for s in range(1, group)]))
                t_all.append(jnp.stack([t] + [swap(t, s) for s in range(1, group)]))
            return jnp.stack(o_all), jnp.stack(t_all)

        o_all, t_all = lax.cond(bound < SAFE_SCORE, bounded, general, first, [list(p) for p in pieces[1:]], t_qkv)
        o_all = o_all.reshape(heads, -1, HEAD)
        t_all = t_all.reshape(heads, -1, HEAD)

        def place(h, own):
            return (h // group) * group + jnp.bitwise_xor(own, h % group)

        t_part, t_res = finish(me, [t_all], place, text, mod[1], w_out, b_out[1:2], w_up, b_up3,
                               w_down, b_down[1:2], 1, w_up.shape[2] // group, True)
        t_sum = lax.psum(t_part, 'cp')
        text_out = (t_res + mod[1, 5] * (t_sum + b_down[1])).astype(jnp.bfloat16)

        image_rows = finish(me, [o_all], place, image, mod[0], w_out, b_out[:1], w_up, b_up3, w_down, b_down[:1], 0, w_up.shape[2], False)
        return image_rows, text_out

    rows_spec = P(('dp', 'cp'), None)
    text_spec = P('dp', None)
    whole = P()
    return jax.shard_map(local, mesh=mesh,
                         in_specs=(rows_spec, text_spec, text_spec, rows_spec, rows_spec) + (whole,) * 11,
                         out_specs=(rows_spec, text_spec), check_vma=False)
```

```python
import functools

import jax
import jax.numpy as jnp
from jax import lax
from jax.experimental import pallas as pl
from jax.experimental.pallas import tpu as pltpu
from jax.sharding import PartitionSpec as P

NORM_EPS = 1e-6
HEAD = 128
LOG2E = 1.4426950408889634
SAFE_SCORE = 60.0
SAFE_POWER = 26.0
MESH = pl.DeviceIdType.MESH


def params(dims):
    return pltpu.CompilerParams(dimension_semantics=("arbitrary",) * dims, vmem_limit_bytes=60 * 2**20)


def cost(flops, moved, trans=0):
    return pl.CostEstimate(flops=flops, bytes_accessed=moved, transcendentals=trans)


def whole_block(shape):
    return pl.BlockSpec(shape, lambda *_: (0,) * len(shape))


def layer_norm(rows):
    mean = jnp.mean(rows, axis=-1, keepdims=True)
    centered = rows - mean
    return centered * lax.rsqrt(jnp.mean(centered * centered, axis=-1, keepdims=True) + NORM_EPS)


def mod_kernel(me_ref, act_ref, w_ref, out_ref):
    out_ref[0] = jnp.dot(act_ref[...], w_ref[0], preferred_element_type=jnp.float32)


def mod_columns(me, activated, w_mod, group):
    branches, hidden, width = w_mod.shape
    share = width // group
    step = share // 3
    rows = activated.shape[0]
    return pl.pallas_call(
        mod_kernel,
        out_shape=jax.ShapeDtypeStruct((branches, rows, share), jnp.float32),
        grid_spec=pltpu.PrefetchScalarGridSpec(
            num_scalar_prefetch=1, grid=(branches, 3),
            in_specs=[whole_block((rows, hidden)),
                      pl.BlockSpec((1, hidden, step), lambda b, n, me: (b, 0, me[0] * 3 + n))],
            out_specs=pl.BlockSpec((1, rows, step), lambda b, n, me: (b, 0, n))),
        compiler_params=params(2), cost_estimate=cost(2 * branches * rows * hidden * share, 2 * branches * hidden * share),
        name="modulate",
    )(me, activated, w_mod)


def head_norm(t, gain):
    x = t.astype(jnp.bfloat16).astype(jnp.float32)
    return x * lax.rsqrt(jnp.mean(x * x, axis=-1, keepdims=True) + NORM_EPS) * gain


def image_qkv_kernel(me_ref, h_ref, *refs, per, tile):
    w_refs, b_refs = refs[:per], refs[per:2 * per]
    gain_ref, cos_ref, sin_ref = refs[2 * per:2 * per + 3]
    outs = refs[2 * per + 3:]
    half, t = pl.program_id(0), pl.program_id(1)
    rows = h_ref.shape[0]

    def run(kind, group):
        weights = jnp.concatenate([w[0] for w in w_refs], axis=1)
        bias = jnp.concatenate([b[0] for b in b_refs], axis=1)
        for m in range(rows // tile):
            sl = pl.ds(m * tile, tile)
            acc = jnp.dot(h_ref[sl, :], weights, preferred_element_type=jnp.float32) + bias
            for i in range(per):
                piece = acc[:, i * HEAD:(i + 1) * HEAD]
                if kind == "v":
                    res = piece
                else:
                    y = head_norm(piece, gain_ref[0])
                    res = y * cos_ref[sl, :] + pltpu.roll(y, HEAD // 2, 1) * sin_ref[sl, :]
                outs[group * per + i][0, sl, :] = res.astype(jnp.bfloat16)

    for group in range(len(outs) // per):
        @pl.when(jnp.logical_and(half == group, t < 2))
        def _():
            run("qk", group)

        @pl.when(jnp.logical_and(half == group, t == 2))
        def _():
            run("v", group)


def image_qkv(me, h, w_qkv, b_qkv, gains, cos, sin, slot, group):
    rows, hidden = h.shape
    heads = hidden // HEAD
    per = 4
    halves = group // per

    def col(i):
        return lambda half, t, me: (0, 0, t * heads + slot * group + jnp.bitwise_xor(me[0], half * per + i))

    def out_map(own):
        def index(half, t, me):
            return (jnp.where(half < own, 0, jnp.where(half == own, t, 2)), 0, 0)
        return index

    return pl.pallas_call(
        functools.partial(image_qkv_kernel, per=per, tile=256),
        out_shape=[jax.ShapeDtypeStruct((3, rows, HEAD), jnp.bfloat16)] * group,
        grid_spec=pltpu.PrefetchScalarGridSpec(
            num_scalar_prefetch=1, grid=(halves, 3),
            in_specs=[whole_block((rows, hidden))]
            + [pl.BlockSpec((1, hidden, HEAD), col(i)) for i in range(per)]
            + [pl.BlockSpec((1, 1, HEAD), col(i)) for i in range(per)]
            + [pl.BlockSpec((1, 1, HEAD), lambda half, t, me: (jnp.minimum(t, 1), 0, 0)),
               whole_block((rows, HEAD)), whole_block((rows, HEAD))],
            out_specs=[pl.BlockSpec((1, rows, HEAD), out_map(s // per)) for s in range(group)]),
        compiler_params=params(2), cost_estimate=cost(2 * rows * hidden * 3 * group * HEAD, 2 * hidden * 3 * group * HEAD),
        name="image_qkv",
    )(me, h, *([w_qkv] * per), *([b_qkv] * per), gains, cos, sin)


def text_qkv_kernel(me_ref, h_ref, w_ref, b_ref, gain_ref, out_ref):
    t = pl.program_id(1)
    acc = jnp.dot(h_ref[...], w_ref[0], preferred_element_type=jnp.float32) + b_ref[0]
    normed = head_norm(acc, gain_ref[0])
    out_ref[0, 0] = jnp.where(t < 2, normed, acc).astype(jnp.bfloat16)


def text_qkv(me, h, w_qkv, b_qkv, gains, slots, group):
    rows, hidden = h.shape
    heads = hidden // HEAD

    def col(j, t, me):
        return (1, 0, t * heads + j * group + me[0])

    return pl.pallas_call(
        text_qkv_kernel,
        out_shape=jax.ShapeDtypeStruct((slots, 3, rows, HEAD), jnp.bfloat16),
        grid_spec=pltpu.PrefetchScalarGridSpec(
            num_scalar_prefetch=1, grid=(slots, 3),
            in_specs=[whole_block((rows, hidden)), pl.BlockSpec((1, hidden, HEAD), col), pl.BlockSpec((1, 1, HEAD), col),
                      pl.BlockSpec((1, 1, HEAD), lambda j, t, me: (jnp.minimum(t, 1), 0, 0))],
            out_specs=pl.BlockSpec((1, 1, rows, HEAD), lambda j, t, me: (j, t, 0, 0))),
        compiler_params=params(2), cost_estimate=cost(2 * rows * hidden * 3 * slots * HEAD, 2 * hidden * 3 * slots * HEAD),
        name="text_qkv",
    )(me, h, w_qkv, b_qkv, gains)


def flip(me, s):
    total = 0
    for k in (1, 2, 4):
        x, y = lax.rem(lax.div(me, k), 2), lax.rem(lax.div(s, k), 2)
        total = total + k * (x + y - 2 * x * y)
    return total


def exchange_kernel(*refs, slots, group, blk, kb):
    first, rest = refs[:group], refs[group:]
    later = [rest[j * group:(j + 1) * group] for j in range(slots - 1)]
    (text, o_recv, t_recv, held, qt, ks, vt, stage, obuf, unscale,
     in_sems, qkv_send, qkv_recv, o_send, o_arrive, t_send, t_arrive) = rest[(slots - 1) * group:]
    i = pl.program_id(0)
    me = lax.axis_index('cp')
    keys = ks.shape[0]
    rows, txt = first[0].shape[1], text.shape[2]
    halves = rows // blk
    n_blocks = keys // blk
    scale2 = LOG2E * HEAD ** -0.5

    def peer(s):
        return {'cp': flip(me, s)}

    def send_rows(j, s):
        return pltpu.make_async_remote_copy(src_ref=later[j - 1][s], dst_ref=held.at[j - 1, s], send_sem=qkv_send.at[j - 1, s],
                                            recv_sem=qkv_recv.at[j - 1, s], device_id=peer(s), device_id_type=MESH)

    def text_copy(slot, j, s):
        if s == 0:
            return pltpu.make_async_copy(obuf.at[slot], t_recv.at[j, 0], t_send.at[j, 0])
        return pltpu.make_async_remote_copy(src_ref=obuf.at[slot], dst_ref=t_recv.at[j, s], send_sem=t_send.at[j, s],
                                            recv_sem=t_arrive.at[j, s], device_id=peer(s), device_id_type=MESH)

    def hand_on(j, s):
        return pltpu.make_async_remote_copy(src_ref=t_recv.at[j, s], dst_ref=t_recv.at[j, s + 1], send_sem=t_send.at[j, s + 1],
                                            recv_sem=t_arrive.at[j, s + 1], device_id=peer(1), device_id_type=MESH)

    def relay(j):
        for s in range(2, group, 2):
            text_copy(0, j, s).wait_recv()
            hand_on(j, s).start()

    def far_copy(slot, j, s, half):
        return pltpu.make_async_remote_copy(src_ref=obuf.at[slot], dst_ref=o_recv.at[j, s, pl.ds(half * blk, blk)],
                                            send_sem=o_send.at[j, s, half], recv_sem=o_arrive.at[j, s, half],
                                            device_id=peer(s), device_id_type=MESH)

    def near_copy(slot, j, half):
        return pltpu.make_async_copy(obuf.at[slot], o_recv.at[j, 0, pl.ds(half * blk, blk)], o_send.at[j, 0, half])

    def send_block(n):
        j, b = lax.div(n, n_blocks), lax.rem(n, n_blocks)
        s = group - 1 - lax.div(b - 1, halves)
        half = lax.rem(b - 1 + halves, halves)

        @pl.when(b == 0)
        def _():
            for t in (0, 1) + tuple(range(2, group, 2)):
                text_copy(n, j, t).start()

        @pl.when(jnp.logical_and(b > 0, b <= (group - 1) * halves))
        def _():
            far_copy(n, j, s, half).start()

        @pl.when(b > (group - 1) * halves)
        def _():
            near_copy(n, j, half).start()

    @pl.when(i == 0)
    def _():
        barrier = pltpu.get_barrier_semaphore()
        for s in range(1, group):
            pl.semaphore_signal(barrier, inc=1, device_id=peer(s), device_id_type=MESH)
        pl.semaphore_wait(barrier, group - 1)
        for j in range(1, slots):
            for s in range(group - 1, 0, -1):
                send_rows(j, s).start()

    @pl.when(i > 0)
    def _():
        send_block(i - 1)

    @pl.when(i == slots * n_blocks - 3)
    def _():
        for j in range(slots - 1):
            relay(j)

    def prepare(j):
        order = [(group - 1 - p) for p in range(group)]
        loads = []
        pos = txt
        for p, s in enumerate(order):
            if j == 0:
                source = first[s]
            elif s == 0:
                source = later[j - 1][0]
            else:
                send_rows(j, s).wait_recv()
                source = held.at[j - 1, s]
            for t in range(3):
                target = ks.at[pl.ds(pos, rows)] if t == 1 else stage.at[p, t // 2]
                copy = pltpu.make_async_copy(source.at[t], target, in_sems.at[p, t])
                copy.start()
                loads.append(copy)
            pos += rows
        qt[0] = text[j, 0].T
        ks[pl.ds(0, txt), :] = text[j, 1]
        for copy in loads:
            copy.wait()
        tv = text[j, 2].astype(jnp.float32)
        top = jnp.max(jnp.abs(tv).reshape(txt // 8, 8, HEAD), axis=0)
        for p in range(group):
            top = jnp.maximum(top, jnp.max(jnp.abs(stage[p, 1].astype(jnp.float32)).reshape(rows // 8, 8, HEAD), axis=0))
        top = jnp.max(jnp.max(top, axis=0, keepdims=True), axis=1, keepdims=True)
        power = jnp.maximum(jnp.ceil(jnp.log2(jnp.maximum(top, 1.0))) - SAFE_POWER, 0.0)
        shrink = jnp.exp2(-power)
        unscale[...] = jnp.broadcast_to(jnp.exp2(power), unscale.shape)
        vt[:, pl.ds(0, txt)] = (tv * shrink).astype(jnp.bfloat16).T
        for p in range(group):
            for c in range(halves):
                sl = pl.ds(c * blk, blk)
                qt[1 + p * halves + c] = stage[p, 0, sl, :].T
                v = (stage[p, 1, sl, :].astype(jnp.float32) * shrink).astype(jnp.bfloat16)
                vt[:, pl.ds(txt + p * rows + c * blk, blk)] = v.T

    for j in range(slots):
        @pl.when(i == j * n_blocks)
        def _():
            prepare(j)

    q = qt[lax.rem(i, n_blocks)]
    acc = jnp.zeros((HEAD, blk), jnp.float32)
    tot = jnp.zeros((8, blk), jnp.float32)
    for c in range(keys // kb):
        sc = jnp.dot(ks[pl.ds(c * kb, kb), :], q, preferred_element_type=jnp.float32)
        p = jnp.exp2(sc * scale2)
        tot = tot + jnp.sum(p.reshape(kb // 8, 8, blk), axis=0)
        acc = acc + jnp.dot(vt[:, pl.ds(c * kb, kb)], p.astype(jnp.bfloat16), preferred_element_type=jnp.float32)
    total = jnp.sum(tot, axis=0, keepdims=True)
    obuf[i] = (acc / total * unscale[0:1, 0:1]).T.astype(jnp.bfloat16)

    @pl.when(i == slots * n_blocks - 1)
    def _():
        send_block(i)
        relay(slots - 1)
        for j in range(slots):
            text_copy(0, j, 0).wait()
            text_copy(0, j, 1).wait()
            for s in range(2, group, 2):
                text_copy(0, j, s).wait_send()
                hand_on(j, s).wait()
            for half in range(halves):
                near_copy(0, j, half).wait()
            for s in range(1, group):
                if j > 0:
                    send_rows(j, s).wait_send()
                for half in range(halves):
                    far_copy(0, j, s, half).wait()


def exchange_attend(first, later, text, blk=512, kb=4352):
    group, slots = len(first), 1 + len(later)
    rows, txt = first[0].shape[1], text.shape[2]
    keys = group * rows + txt
    any_space = pl.BlockSpec(memory_space=pl.ANY)
    dma = pltpu.SemaphoreType.DMA
    bf16 = jnp.bfloat16
    o_recv, t_recv, _ = pl.pallas_call(
        functools.partial(exchange_kernel, slots=slots, group=group, blk=blk, kb=kb),
        out_shape=[jax.ShapeDtypeStruct((slots, group, rows, HEAD), bf16), jax.ShapeDtypeStruct((slots, group, txt, HEAD), bf16),
                   jax.ShapeDtypeStruct((slots - 1, group, 3, rows, HEAD), bf16)],
        grid=(slots * (keys // blk),),
        in_specs=[any_space] * (group * slots) + [whole_block(text.shape)],
        out_specs=[any_space] * 3,
        scratch_shapes=[pltpu.VMEM((keys // blk, HEAD, blk), bf16), pltpu.VMEM((keys, HEAD), bf16), pltpu.VMEM((HEAD, keys), bf16),
                        pltpu.VMEM((group, 2, rows, HEAD), bf16), pltpu.VMEM((slots * (keys // blk), blk, HEAD), bf16), pltpu.VMEM((8, HEAD), jnp.float32),
                        dma((group, 3)), dma((slots - 1, group)), dma((slots - 1, group)),
                        dma((slots, group, rows // blk)), dma((slots, group, rows // blk)), dma((slots, group)), dma((slots, group))],
        compiler_params=pltpu.CompilerParams(dimension_semantics=("arbitrary",), vmem_limit_bytes=60 * 2**20,
                                             collective_id=0, has_side_effects=True),
        cost_estimate=cost(slots * 4 * keys * keys * HEAD, slots * 8 * keys * HEAD, slots * keys * keys),
        name="exchange_attend",
    )(*first, *[piece for pieces in later for piece in pieces], text)
    return o_recv, t_recv


def attend_kernel(*refs, n_src, blk):
    srcs, tref = refs[:n_src], refs[n_src]
    o_ref, tout = refs[n_src + 1:n_src + 3]
    qt, ks, vt = refs[n_src + 3:]
    b = pl.program_id(0)
    keys = ks.shape[0]
    rows, txt = srcs[0].shape[1], tref.shape[1]
    scale2 = LOG2E * HEAD ** -0.5

    @pl.when(b == 0)
    def _():
        pos = 0
        for ref in (tref,) + tuple(srcs):
            for c in range(ref.shape[1] // blk):
                sl = pl.ds(c * blk, blk)
                qt[pos // blk] = ref[0, sl, :].T
                ks[pl.ds(pos, blk), :] = ref[1, sl, :]
                vt[:, pl.ds(pos, blk)] = ref[2, sl, :].T
                pos += blk

    q = qt[b]

    def body(i, carry):
        acc, tot, peak = carry
        st = pl.multiple_of(i * blk, blk)
        sc = jnp.dot(ks[pl.ds(st, blk), :], q, preferred_element_type=jnp.float32) * scale2
        new = jnp.maximum(peak, jnp.max(sc, axis=0, keepdims=True))
        p = jnp.exp2(sc - new)
        factor = jnp.exp2(peak - new)
        tot = tot * factor + jnp.sum(p, axis=0, keepdims=True)
        acc = acc * factor + jnp.dot(vt[:, pl.ds(st, blk)], p.astype(jnp.bfloat16), preferred_element_type=jnp.float32)
        return acc, tot, new

    start = (jnp.zeros((HEAD, blk), jnp.float32), jnp.zeros((1, blk), jnp.float32), jnp.full((1, blk), -jnp.inf, jnp.float32))
    acc, tot, _ = lax.fori_loop(0, keys // blk, body, start)
    val = (acc / tot).T.astype(jnp.bfloat16)

    @pl.when(b == 0)
    def _():
        tout[...] = val

    @pl.when(b > 0)
    def _():
        o_ref[pl.ds(pl.multiple_of((b - 1) * blk, blk), blk), :] = val


def attend(srcs, text, blk=512):
    n_src, rows, txt = len(srcs), srcs[0].shape[1], text.shape[1]
    keys = n_src * rows + txt
    return pl.pallas_call(
        functools.partial(attend_kernel, n_src=n_src, blk=blk),
        out_shape=[jax.ShapeDtypeStruct((n_src * rows, HEAD), jnp.bfloat16), jax.ShapeDtypeStruct((txt, HEAD), jnp.bfloat16)],
        grid=(keys // blk,),
        in_specs=[whole_block((3, rows, HEAD))] * n_src + [whole_block((3, txt, HEAD))],
        out_specs=[whole_block((n_src * rows, HEAD)), whole_block((txt, HEAD))],
        scratch_shapes=[pltpu.VMEM((keys // blk, HEAD, blk), jnp.bfloat16), pltpu.VMEM((keys, HEAD), jnp.bfloat16),
                        pltpu.VMEM((HEAD, keys), jnp.bfloat16)],
        compiler_params=params(1), cost_estimate=cost(4 * keys * keys * HEAD, 8 * keys * HEAD, keys * keys), name="attend",
    )(*srcs, text)


def norm_kernel(x_ref, shift_ref, scale_ref, out_ref):
    out_ref[...] = (layer_norm(x_ref[...].astype(jnp.float32)) * (1.0 + scale_ref[...]) + shift_ref[...]).astype(jnp.bfloat16)


def modulated_norm(x, shift, scale):
    rows, hidden = x.shape
    block = pl.BlockSpec((128, hidden), lambda i: (i, 0))
    return pl.pallas_call(
        norm_kernel, out_shape=jax.ShapeDtypeStruct(x.shape, jnp.bfloat16), grid=(rows // 128,),
        in_specs=[block, whole_block((1, hidden)), whole_block((1, hidden))], out_specs=block,
        compiler_params=params(1), cost_estimate=cost(10 * rows * hidden, 4 * rows * hidden), name="norm",
    )(x, shift, scale)


def finish_kernel(me_ref, *refs, n_o, heads, n_proj, n_ff, step, tile, place, split):
    o_refs = refs[:n_o]
    x_ref, w_out, w_up, w_down, mod_ref, b_out, b_up, b_down = refs[n_o:n_o + 8]
    if split:
        part_ref, rows_buf, r_ref, in_sems, out_sems = refs[n_o + 8:]
    else:
        y_out, rows_buf, r_ref, in_sems, out_sems = refs[n_o + 8:]
    i = pl.program_id(0)
    rows = r_ref.shape[0]
    tiles = [pl.ds(m * tile, tile) for m in range(rows // tile)]

    def fetch(h):
        spot = pl.multiple_of(place(h, me_ref[0]) * HEAD, HEAD)
        source = o_refs[h] if n_o > 1 else o_refs[0].at[h]
        return pltpu.make_async_copy(source, rows_buf.at[:, pl.ds(spot, HEAD)], in_sems.at[h])

    @pl.when(i == 0)
    def _():
        for h in range(heads):
            fetch(h).start()
        for h in range(heads):
            fetch(h).wait()

    @pl.when(i < n_proj)
    def _():
        cols = pl.ds(pl.multiple_of(i * step, step), step)
        for sl in tiles:
            acc = jnp.dot(rows_buf[sl, :], w_out[0], preferred_element_type=jnp.float32)
            r_ref[sl, cols] = x_ref[sl, :].astype(jnp.float32) + mod_ref[2, :, cols] * (acc + b_out[:, cols])

    def y_copy(m):
        return pltpu.make_async_copy(rows_buf.at[tiles[m]], y_out.at[tiles[m]], out_sems.at[m])

    def feed(first, last):
        for m, sl in enumerate(tiles):
            if first:
                res = r_ref[sl, :]
                h = (layer_norm(res) * (1.0 + mod_ref[4]) + mod_ref[3]).astype(jnp.bfloat16)
                rows_buf[sl, :] = h
            else:
                h = rows_buf[sl, :]
            u = jnp.dot(h, w_up[0], preferred_element_type=jnp.float32) + b_up[0]
            u = jax.nn.gelu(u, approximate=True).astype(jnp.bfloat16)
            part = jnp.dot(u, w_down[0], preferred_element_type=jnp.float32)
            if split:
                if first:
                    part_ref[sl, :] = res * (1.0 / split) + mod_ref[5] * part
                else:
                    part_ref[sl, :] += mod_ref[5] * part
                continue
            base = res + mod_ref[5] * b_down[...] if first else r_ref[sl, :]
            total = base + mod_ref[5] * part
            if last:
                rows_buf[sl, :] = total.astype(jnp.bfloat16)
                y_copy(m).start()
            else:
                r_ref[sl, :] = total
        if last and not split:
            for m in range(len(tiles)):
                y_copy(m).wait()

    final = n_proj + n_ff - 1

    @pl.when(i == n_proj)
    def _():
        feed(True, False)

    @pl.when(jnp.logical_and(i > n_proj, i < final))
    def _():
        feed(False, False)

    @pl.when(i == final)
    def _():
        feed(False, True)


def finish(me, attended, place, x, mod, w_out, b_out, w_up, b_up, w_down, b_down, branch, share, split):
    rows, hidden = x.shape
    step, tile = 512, min(rows, 1024)
    n_proj, n_ff = hidden // step, share // step
    n_o, heads = len(attended), hidden // HEAD

    def proj(i):
        return jnp.minimum(i, n_proj - 1)

    def ff(i, me):
        at = jnp.clip(i - n_proj, 0, n_ff - 1)
        return at + me[0] * n_ff if split else at

    any_space = pl.BlockSpec(memory_space=pl.ANY)
    if split:
        out_shape = jax.ShapeDtypeStruct((rows, hidden), jnp.float32)
        out_specs = whole_block((rows, hidden))
    else:
        out_shape = jax.ShapeDtypeStruct((rows, hidden), jnp.bfloat16)
        out_specs = any_space
    return pl.pallas_call(
        functools.partial(finish_kernel, n_o=n_o, heads=heads, n_proj=n_proj, n_ff=n_ff, step=step, tile=tile, place=place, split=split),
        out_shape=out_shape,
        grid_spec=pltpu.PrefetchScalarGridSpec(
            num_scalar_prefetch=1, grid=(n_proj + n_ff,),
            in_specs=[any_space] * n_o
            + [pl.BlockSpec((rows, step), lambda i, me: (0, proj(i))),
               pl.BlockSpec((1, hidden, step), lambda i, me: (branch, 0, proj(i))),
               pl.BlockSpec((1, hidden, step), lambda i, me: (branch, 0, ff(i, me))),
               pl.BlockSpec((1, step, hidden), lambda i, me: (branch, ff(i, me), 0)),
               whole_block((6, 1, hidden)), whole_block((1, hidden)),
               pl.BlockSpec((1, 1, step), lambda i, me: (branch, 0, ff(i, me))), whole_block((1, hidden))],
            out_specs=out_specs,
            scratch_shapes=[pltpu.VMEM((rows, hidden), jnp.bfloat16), pltpu.VMEM((rows, hidden), jnp.float32),
                            pltpu.SemaphoreType.DMA((heads,)), pltpu.SemaphoreType.DMA((rows // tile,))]),
        compiler_params=params(1),
        cost_estimate=cost(2 * rows * hidden * (hidden + 2 * share), 2 * hidden * (hidden + 2 * share) + 8 * rows * hidden),
        name="finish_text" if split else "finish_image",
    )(me, *attended, x, w_out, w_up, w_down, mod, b_out, b_up, b_down)


def solution(mesh):
    group = mesh.shape['cp']

    def local(image, text, cond_vec, rope_cos, rope_sin, w_mod, b_mod, w_qkv, b_qkv, qk_gain, w_out, b_out, w_up, b_up, w_down, b_down):
        hidden = image.shape[-1]
        heads = hidden // HEAD
        slots = heads // group
        me = jnp.reshape(lax.axis_index('cp'), (1,)).astype(jnp.int32)

        activated = jax.nn.silu(cond_vec.astype(jnp.float32)).astype(jnp.bfloat16)
        columns = mod_columns(me, jnp.broadcast_to(activated, (16, hidden)), w_mod, group)[:, 0, :]
        mod = lax.all_gather(columns, 'cp', axis=1, tiled=True) + b_mod
        mod = mod.reshape(2, 6, 1, hidden)

        b_qkv3 = b_qkv.reshape(2, 1, -1)
        b_up3 = b_up.reshape(2, 1, -1)
        gains = qk_gain.reshape(2, 2, 1, HEAD)
        cos = jnp.concatenate([rope_cos, rope_cos], axis=1)
        sin = jnp.concatenate([-rope_sin, rope_sin], axis=1)
        peaks = jnp.max(jnp.abs(qk_gain), axis=(0, 2))
        bound = 1.02 * HEAD ** 0.5 * peaks[0] * peaks[1]

        h_img = modulated_norm(image, mod[0, 0], mod[0, 1])
        h_txt = modulated_norm(text, mod[1, 0], mod[1, 1])

        def swap(value, bits):
            return lax.ppermute(value, 'cp', [(i, i ^ bits) for i in range(group)])

        pieces = [image_qkv(me, h_img, w_qkv, b_qkv3, gains[0], cos, sin, j, group) for j in range(slots)]
        first = [pieces[0][0]] + [swap(pieces[0][s], s) for s in range(1, group)]
        t_qkv = text_qkv(me, h_txt, w_qkv, b_qkv3, gains[1], slots, group)

        def bounded(first, later, t_qkv):
            return exchange_attend(first, later, t_qkv)

        def general(first, later, t_qkv):
            o_all, t_all = [], []
            for j in range(slots):
                srcs = first if j == 0 else [later[j - 1][0]] + [swap(later[j - 1][s], s) for s in range(1, group)]
                o, t = attend(srcs, t_qkv[j])
                o = o.reshape(group, -1, HEAD)
                o_all.append(jnp.stack([o[0]] + [swap(o[s], s) for s in range(1, group)]))
                t_all.append(jnp.stack([t] + [swap(t, s) for s in range(1, group)]))
            return jnp.stack(o_all), jnp.stack(t_all)

        o_all, t_all = lax.cond(bound < SAFE_SCORE, bounded, general, first, [list(p) for p in pieces[1:]], t_qkv)
        o_all = o_all.reshape(heads, -1, HEAD)
        t_all = t_all.reshape(heads, -1, HEAD)

        def place(h, own):
            return (h // group) * group + jnp.bitwise_xor(own, h % group)

        t_part = finish(me, [t_all], place, text, mod[1], w_out, b_out[1:2], w_up, b_up3,
                               w_down, b_down[1:2], 1, w_up.shape[2] // group, group)
        text_out = (lax.psum(t_part, 'cp') + mod[1, 5] * b_down[1]).astype(jnp.bfloat16)

        image_rows = finish(me, [o_all], place, image, mod[0], w_out, b_out[:1], w_up, b_up3, w_down, b_down[:1], 0, w_up.shape[2], 0)
        return image_rows, text_out

    rows_spec = P(('dp', 'cp'), None)
    text_spec = P('dp', None)
    whole = P()
    return jax.shard_map(local, mesh=mesh,
                         in_specs=(rows_spec, text_spec, text_spec, rows_spec, rows_spec) + (whole,) * 11,
                         out_specs=(rows_spec, text_spec), check_vma=False)
```
